512 devices in a mesh: rep: 32 (over x, z), tp: 16 (over y, core).
Axes of the slice: x: 4, y: 8, z: 8, core: 2. Of those that a mesh axis runs over, the one named last changes fastest.
Arguments:
- prompt_queries: bfloat16 [15872, 4096], P('rep', 'tp'), parts along dimension 0, may hold values from -240 to 240
- prompt_entries: bfloat16 [64, 496, 512], P('rep', 'tp'), parts along dimension 0, may hold values from -6 to 6
- history_cache: bfloat16 [64, 1024, 512], P('rep', 'tp'), parts along dimension 0, may hold values from -6 to 6
- decode_queries: bfloat16 [512, 4096], P('rep', 'tp'), parts along dimension 0, may hold values from -240 to 240
- decode_entries: bfloat16 [64, 16, 512], P('rep'), parts along dimension 0, may hold values from -6 to 6
- decode_cache: bfloat16 [64, 16, 768, 512], P('rep', None, 'tp'), parts along dimension 0, may hold values from -6 to 6
- decode_lengths: int32 [512], P('rep'), parts along dimension 0, may hold values from 1 to 768
- prompt_start: int32 [32], P('rep'), parts along dimension 0, may hold values from 512 to 1024
- out_weight: bfloat16 [4096, 4096], P('tp'), may hold values from -0.09375 to 0.09375
- residual: bfloat16 [512, 131072], P('tp', 'rep'), parts along dimension 1, may hold values from -4 to 4
- norm_gain: float32 [4096], replicated, may hold values from 0.5 to 1.5
Outputs:
- new_residual: bfloat16 [512, 131072], P('tp', 'rep'), parts along dimension 1
- normed: bfloat16 [512, 131072], P('tp', 'rep'), parts along dimension 1
The draws below stay inside these ranges and needn't reach their ends.
There are 32 independent parts, one for each index of `rep`. The reference program is written for one: setup_inputs(seed, part) draws one part's arguments, and reference() takes and returns one part's arrays. A program takes and returns all parts, laid end to end along the dimension named above; an argument that names none is the same for every part. Nothing has to cross between parts.
Inputs may be any that keep to these rules, and one draw needn't show every extreme that they name: The rows of history_cache at and past prompt_start are not read. `decode_lengths`: rows of decode_cache at and past a request's length are not read.
All inputs are finite; a program needn't handle non-finite values.
Results may differ from the reference program's by a relative error of at most 0.017.
Values may be sent and summed in bfloat16 or wider, within the bound.
A program may use at most 64 MiB of HBM per device.

```python
import jax
import jax.numpy as jnp
from jax import lax

D = 4096
HEADS = 32
KV_HEADS = 4
HEAD_DIM = 128
PROMPT = 496
DECODE = 16
HISTORY = 1024
CACHE = 768
TOKENS = 512
N_TP = 16


def spread_queries(key, row_count):
    values = jnp.clip(2.0 * jax.random.normal(key, (row_count, HEADS * HEAD_DIM), jnp.float32), -12.0, 12.0)
    return values.astype(jnp.bfloat16)


def draw_prompt_queries(key, part):
    return spread_queries(jax.random.fold_in(key, 3), PROMPT)


def draw_decode_queries(key, part):
    return spread_queries(jax.random.fold_in(key, 5), DECODE)


def place_ends(entries, key, least, high):
    shape = entries.shape
    spot = [jax.random.randint(jax.random.fold_in(key, axis), (), 0, shape[axis]) for axis in range(len(shape))]
    entries = entries.at[tuple(spot)].set(least)
    longest = shape.index(max(shape))
    spot[longest] = (spot[longest] + 1) % shape[longest]
    return entries.at[tuple(spot)].set(high)


def shard_levels(stream_key, shape, split, least, top_value):
    gain = 1.0
    for dim, shards_of in split:
        heights = jax.random.uniform(jax.random.fold_in(jax.random.fold_in(stream_key, 6), dim), (shards_of,), jnp.float32, least / len(split), top_value / len(split))
        gain = gain * jnp.repeat(jnp.exp(heights), shape[dim] // shards_of).reshape((-1,) + (1,) * (len(shape) - 1 - dim))
    return gain


def bell_draw(own_key, extent, deviation, limit, cuts=(), kind=jnp.bfloat16):
    values = jax.random.normal(own_key, extent, jnp.float32) * deviation
    if len(cuts) > 0:
        values = shard_levels(own_key, extent, cuts, -0.22, 0.18) * values
    return jnp.clip(values, min=-limit, max=limit).astype(kind)


def setup_inputs(seed: int = 0, part: int = 0) -> dict:
    key_list = jax.random.split(jax.random.key(seed), 12)
    part_splits = jax.random.split(jax.random.fold_in(key_list[11], part), 12)
    return {
        "prompt_queries": draw_prompt_queries(jax.random.fold_in(jax.random.fold_in(key_list[11], part), 71), part),
        "prompt_entries": bell_draw(part_splits[1], (2, PROMPT, KV_HEADS * HEAD_DIM), 1.0, 6.0, ((1, 16),)),
        "history_cache": bell_draw(part_splits[2], (2, HISTORY, KV_HEADS * HEAD_DIM), 1.0, 6.0, ((1, 16),)),
        "decode_queries": draw_decode_queries(jax.random.fold_in(jax.random.fold_in(key_list[11], part), 71), part),
        "decode_entries": bell_draw(part_splits[4], (2, DECODE, KV_HEADS * HEAD_DIM), 1.0, 6.0),
        "decode_cache": bell_draw(part_splits[5], (2, DECODE, CACHE, KV_HEADS * HEAD_DIM), 1.0, 6.0, ((2, 16),)),
        "decode_lengths": place_ends(jax.random.randint(part_splits[6], (DECODE,), 1, CACHE + 1), jax.random.fold_in(part_splits[6], 1), 1, CACHE).astype(jnp.int32),
        "prompt_start": jax.random.randint(part_splits[7], (1,), HISTORY // 2, HISTORY + 1).astype(jnp.int32),
        "out_weight": bell_draw(key_list[8], (HEADS * HEAD_DIM, D), (HEADS * HEAD_DIM) ** -0.5, 0.09375, ((0, 16),)),
        "residual": bell_draw(part_splits[9], (TOKENS, D), 0.3, 4.0, ((0, 16),)),
        "norm_gain": jnp.clip(1.0 + 0.1 * jax.random.normal(key_list[10], (D,), jnp.float32), 0.5, 1.5),
    }


def weighted(scores, valid):
    masked = jnp.where(valid, scores, -jnp.inf)
    highest = lax.optimization_barrier(jnp.max(masked, axis=-1, keepdims=True))
    weights = jnp.where(valid, jnp.exp(scores - highest), 0.0)
    totals = lax.optimization_barrier(jnp.sum(weights, axis=-1))
    rounded = lax.optimization_barrier(weights.astype(jnp.bfloat16)).astype(jnp.float32)
    return (rounded, totals)

def prompt_attention(prompt_queries, prompt_entries, history_cache, start):
    group = HEADS // KV_HEADS
    scale = HEAD_DIM ** (-0.5)
    keys = jnp.concatenate([history_cache[0], prompt_entries[0]], axis=0).reshape(HISTORY + PROMPT, KV_HEADS, HEAD_DIM)
    values = jnp.concatenate([history_cache[1], prompt_entries[1]], axis=0).reshape(HISTORY + PROMPT, KV_HEADS, HEAD_DIM)
    queries = prompt_queries.reshape(PROMPT, KV_HEADS, group, HEAD_DIM)
    slots = jnp.arange(HISTORY + PROMPT, dtype=jnp.int32)[None, :]
    places = jnp.arange(PROMPT, dtype=jnp.int32)[:, None]
    valid = jnp.where(slots < HISTORY, slots < start, slots - HISTORY <= places)

    def one_head(inputs):
        query_block, key_block, value_block = inputs
        scores = jnp.einsum('tgd,pd->tgp', query_block.astype(jnp.float32), key_block.astype(jnp.float32)) * scale
        weights, totals = weighted(scores, valid[:, None, :])
        summed = jnp.einsum('tgp,pd->tgd', weights, value_block.astype(jnp.float32))
        return (summed / totals[..., None]).astype(jnp.bfloat16)
    outputs = lax.map(one_head, (queries.transpose(1, 0, 2, 3), keys.transpose(1, 0, 2), values.transpose(1, 0, 2)))
    return outputs.transpose(1, 0, 2, 3).reshape(PROMPT, HEADS * HEAD_DIM)

def decode_attention(decode_queries, decode_entries, decode_cache, lengths):
    group = HEADS // KV_HEADS
    scale = HEAD_DIM ** (-0.5)
    keys = jnp.concatenate([decode_cache[0].reshape(DECODE, CACHE, KV_HEADS, HEAD_DIM), decode_entries[0].reshape(DECODE, 1, KV_HEADS, HEAD_DIM)], axis=1)
    values = jnp.concatenate([decode_cache[1].reshape(DECODE, CACHE, KV_HEADS, HEAD_DIM), decode_entries[1].reshape(DECODE, 1, KV_HEADS, HEAD_DIM)], axis=1)
    slots = jnp.arange(CACHE + 1, dtype=jnp.int32)[None, :]
    valid = (slots < lengths[:, None]) | (slots == CACHE)
    queries = decode_queries.reshape(DECODE, KV_HEADS, group, HEAD_DIM)
    scores = jnp.einsum('bkgd,bpkd->bkgp', queries.astype(jnp.float32), keys.astype(jnp.float32)) * scale
    weights, totals = weighted(scores, valid[:, None, None, :])
    summed = jnp.einsum('bkgp,bpkd->bkgd', weights, values.astype(jnp.float32))
    return (summed / totals[..., None]).astype(jnp.bfloat16).reshape(DECODE, HEADS * HEAD_DIM)

def reference(prompt_queries, prompt_entries, history_cache, decode_queries, decode_entries, decode_cache, decode_lengths, prompt_start, out_weight, residual, norm_gain):
    prompt_out = prompt_attention(prompt_queries, prompt_entries, history_cache, prompt_start[0])
    decode_out = decode_attention(decode_queries, decode_entries, decode_cache, decode_lengths)
    attended = jnp.concatenate([prompt_out, decode_out], axis=0)
    width = HEADS * HEAD_DIM // N_TP
    projected = jnp.zeros((TOKENS, D), jnp.float32)
    for block in range(N_TP):
        partial_value = jnp.dot(attended[:, block * width:(block + 1) * width], out_weight[block * width:(block + 1) * width], preferred_element_type=jnp.float32)
        projected = projected + lax.optimization_barrier(partial_value.astype(jnp.bfloat16)).astype(jnp.float32)
    hidden = residual.astype(jnp.float32) + projected
    mean_square = lax.optimization_barrier(jnp.mean(hidden * hidden, axis=-1, keepdims=True))
    normed = (hidden * lax.rsqrt(mean_square + 1e-05) * norm_gain).astype(jnp.bfloat16)
    return (hidden.astype(jnp.bfloat16), normed)
```

```python
import jax
import jax.numpy as jnp
from jax import lax
from jax.experimental import pallas as pl
from jax.experimental.pallas import tpu as pltpu
from jax.sharding import PartitionSpec as P

HEAD_DIM = 128
CHIPS = 8
GROUP = 16
SUBS = 4
MESH = pl.DeviceIdType.MESH
LOWEST = -(2.0**100)
FACTOR = HEAD_DIM**-0.5 * 1.4426950408889634
NEVER = 1 << 20

f32 = jnp.float32
bf16 = jnp.bfloat16


def dot_t(a, b):
    return lax.dot_general(a, b, (((1,), (1,)), ((), ())), preferred_element_type=f32)


def iota(shape, dim):
    return lax.broadcasted_iota(jnp.int32, shape, dim)


def kernel(
    start_ref, lengths_ref, pq, pe, hist, dq, de, dc, w, res, gain,
    out_res, out_norm,
    stage, pbuf, kv, qbuf, dbuf, qd, wbuf, resbuf, gainbuf, fresh,
    part_send, part_recv, part_mine, dec_send, dec_recv, att, rs_send, rs_recv, hid,
    local_sem, qd_ssem, qd_rsem, kv_ssem, kv_rsem, pair_ssem, pair_rsem,
    part_ssem, part_rsem, dec_ssem, dec_rsem, rs_ssem, rs_rsem,
):
    t = lax.axis_index("tp")
    y = t // 2
    c = t % 2
    head = y // 2
    half = y // 4
    partner = 2 * y + 1 - c
    span = hist.shape[1]
    rows = pq.shape[0]
    width = rs_send.shape[-1]

    def local(src, dst, n):
        return pltpu.make_async_copy(src, dst, local_sem.at[n])

    def remote(src, dst, ssem, rsem, device):
        return pltpu.make_async_remote_copy(
            src_ref=src, dst_ref=dst, send_sem=ssem, recv_sem=rsem,
            device_id={"tp": device}, device_id_type=MESH,
        )

    def lanes(index, size):
        return pl.ds(pl.multiple_of(index * size, size), size)

    locals_ = [
        local(hist, stage.at[:, pl.ds(0, span), :], 0),
        local(pe, pbuf, 1),
        local(hist.at[:, :, lanes(head, 128)], kv.at[:, y, pl.ds(0, span), :], 2),
        local(dc.at[:, :, :, lanes(c, 256)], dbuf.at[c], 3),
    ]
    for i in range(2):
        columns = pl.ds(128 * i, 128)
        locals_.append(local(pq.at[:, columns], qbuf.at[2 * c + i, pl.ds(0, rows), :], 4 + i))
        locals_.append(local(dq.at[:, columns], qbuf.at[2 * c + i, pl.ds(rows, 16), :], 6 + i))
    locals_ += [
        local(de.at[:, :, lanes(head, 128)], fresh, 8),
        local(w, wbuf.at[pl.ds(pl.multiple_of(256 * c, 256), 256), :], 9),
        local(res, resbuf, 10),
        local(gain, gainbuf, 11),
    ]
    for copy in locals_:
        copy.start()

    barrier = pltpu.get_barrier_semaphore()
    for k in range(1, GROUP):
        pl.semaphore_signal(
            barrier, inc=1, device_id={"tp": (t + k) % GROUP}, device_id_type=MESH
        )

    locals_[0].wait()
    locals_[1].wait()
    entries = pe.shape[1]
    for i in range(2):
        stage[i, span : span + 32, :] = jnp.concatenate(
            [pbuf[i], jnp.zeros((32 - entries, pbuf.shape[2]), bf16)], axis=0
        )
    for i in range(2):
        kv[i, y, span : span + 32, :] = stage[i, span : span + 32, lanes(head, 128)]
    rs_recv[0, 0, 2:4] = jnp.zeros((2, 32, width), bf16)
    rs_recv[1, 0, 0:2] = jnp.zeros((2, 32, width), bf16)
    pl.semaphore_wait(barrier, GROUP - 1)

    slot = t - 8 * half
    qd_copies = []
    for k in range(1, CHIPS):
        copy = remote(dq, qd.at[slot], qd_ssem.at[k], qd_rsem.at[slot], 2 * ((y + k) % CHIPS) + half)
        copy.start()
        qd_copies.append(copy)
    qd_pair = remote(dq, qd.at[slot], qd_ssem.at[0], qd_rsem.at[slot], partner)
    qd_own = pltpu.make_async_copy(dq, qd.at[slot], qd_rsem.at[slot])

    @pl.when(c == half)
    def _():
        qd_own.start()

    @pl.when(c != half)
    def _():
        qd_pair.start()

    kv_copies = []
    for k in (4, 3, 5, 2, 6, 1, 7):
        there = (y + k) % CHIPS
        copy = remote(
            stage.at[:, :, lanes(there // 2, 128)], kv.at[:, y], kv_ssem.at[k], kv_rsem.at[y],
            2 * there + c,
        )
        copy.start()
        kv_copies.append(copy)

    pairs = [remote(dc.at[:, :, :, lanes(1 - c, 256)], dbuf.at[c], pair_ssem.at[0], pair_rsem.at[0], partner)]
    for i in range(2):
        columns = pl.ds(128 * i, 128)
        pairs.append(
            remote(pq.at[:, columns], qbuf.at[2 * c + i, pl.ds(0, rows), :],
                   pair_ssem.at[1 + i], pair_rsem.at[1 + i], partner)
        )
        pairs.append(
            remote(dq.at[:, columns], qbuf.at[2 * c + i, pl.ds(rows, 16), :],
                   pair_ssem.at[3 + i], pair_rsem.at[3 + i], partner)
        )
    pairs.append(
        remote(w, wbuf.at[pl.ds(pl.multiple_of(256 * c, 256), 256), :],
               pair_ssem.at[5], pair_rsem.at[5], partner)
    )
    for copy in pairs:
        copy.start()

    row_b = iota((128, 1), 0) & 15
    limit = jnp.zeros((128, 1), jnp.int32)
    for b in range(16):
        limit = jnp.where(row_b == b, lengths_ref[b], limit)
    col = iota((1, 768), 1)
    col_b = (col * 1366) >> 16
    col_p = col - 48 * col_b
    lane = iota((128, 128), 1)

    locals_[3].wait()
    pairs[0].wait_recv()
    for s in range(8):
        pltpu.make_async_copy(dq, qd.at[s], qd_rsem.at[s]).wait()
    for g in range(2):
        columns = slice(128 * g, 128 * g + 128)
        q = jnp.concatenate(
            [qd[4 * g + n, :, 128 * i : 128 * i + 128] for n in range(4) for i in range(2)], axis=0
        )
        scores = []
        for core in range(2):
            keys = dbuf[core, 0, :, :, columns].reshape(768, 128)
            places = (2 * y + core) * 48 + col_p
            valid = (col_b == row_b) & (places < limit)
            scores.append(jnp.where(valid, dot_t(q, keys), LOWEST))
        top = jnp.maximum(*[jnp.max(s, axis=1, keepdims=True) for s in scores])
        top = top.astype(bf16).astype(f32)
        total = jnp.zeros((128, 1), f32)
        summed = jnp.zeros((128, 128), f32)
        for core in range(2):
            weights = jnp.exp2((scores[core] - top) * FACTOR)
            total += jnp.sum(weights, axis=1, keepdims=True)
            values = dbuf[core, 1, :, :, columns].reshape(768, 128)
            summed += jnp.dot(weights.astype(bf16), values, preferred_element_type=f32)
        stats = jnp.where(lane < 64, top, total).astype(bf16)
        summed = summed.astype(bf16)
        for n in range(2):
            dec_send[2 * g + n, 0] = summed[64 * n : 64 * n + 64]
            dec_send[2 * g + n, 1] = stats[64 * n : 64 * n + 64]
    dec_copies = []
    for j in range(4):
        copy = remote(dec_send.at[j], dec_recv.at[y], dec_ssem.at[j], dec_rsem.at[y], 2 * (4 * c + j) + 1)
        dec_copies.append(copy)
        stays = (c == 1) & (y == 4 + j)

        @pl.when(stays)
        def _():
            dec_recv[y] = dec_send[j]

        @pl.when(jnp.logical_not(stays))
        def _():
            copy.start()

    block = (col * 683) >> 16
    place = col - 96 * block
    owner = 2 * block + c
    start = start_ref[0]
    from_history = jnp.where(owner * span + place < start, -1, NEVER)
    from_prompt = jnp.where(place < span + entries, owner * entries + place - span, NEVER)
    first_row = jnp.where(place < span, from_history, from_prompt)
    row32 = iota((128, 1), 0) & 31

    for n in (2, 4, 5, 6, 7):
        locals_[n].wait()
    for copy in pairs[1:5]:
        copy.wait_recv()
    for k in range(1, CHIPS):
        there = (y + k) % CHIPS
        pltpu.make_async_copy(kv.at[:, there], kv.at[:, there], kv_rsem.at[there]).wait()

    def attend(row):
        row = pl.multiple_of(row, 32)
        q = qbuf[:, pl.ds(row, 32), :].reshape(128, 128)
        keys = kv[0].reshape(768, 128)
        values = kv[1].reshape(768, 128)
        scores = jnp.where(first_row <= row + row32, dot_t(q, keys), LOWEST)
        top = jnp.max(scores, axis=1, keepdims=True)
        weights = jnp.exp2((scores - top) * FACTOR)
        total = jnp.sum(weights, axis=1, keepdims=True)
        summed = jnp.dot(weights.astype(bf16), values, preferred_element_type=f32)
        return summed, jnp.where(lane < 64, top, total)

    def part_copy(i):
        return remote(part_send.at[i], part_recv.at[i], part_ssem.at[i], part_rsem.at[i], partner)

    def attend_both(i, d, slot):
        summed, stats = attend(64 * d + 32 * (1 - c))
        part_send[i, 0] = summed
        part_send[i, 1] = stats
        part_copy(i).start()
        summed, stats = attend(64 * d + 32 * c)
        part_mine[slot, 0] = summed
        part_mine[slot, 1] = stats

    def decode_rows(slot):
        for s in range(CHIPS):
            @pl.when(jnp.logical_not((y == s) & (y >= 4)))
            def _():
                pltpu.make_async_copy(dec_send.at[0], dec_recv.at[s], dec_rsem.at[s]).wait()
        query = qbuf[:, rows : rows + 16, :].astype(f32)
        key = fresh[0].astype(f32)
        value = fresh[1].astype(f32)
        own = jnp.sum(query * key[None], axis=-1, keepdims=True).reshape(64, 1)
        value = jnp.concatenate([value] * 4, axis=0)
        tops = [dec_recv[s, 1, :, 0:1].astype(f32) for s in range(CHIPS)]
        top = own
        for s in range(CHIPS):
            top = jnp.maximum(top, tops[s])
        own_weight = jnp.exp2((own - top) * FACTOR)
        total = own_weight
        summed = own_weight.astype(bf16).astype(f32) * value
        for s in range(CHIPS):
            factor = jnp.exp2((tops[s] - top) * FACTOR)
            total += factor * dec_recv[s, 1, :, 64:65].astype(f32)
            summed += factor * dec_recv[s, 0].astype(f32)
        out = (summed / total).astype(bf16)
        for n in range(4):
            att[slot, 16:32, 128 * n : 128 * n + 128] = out[16 * n : 16 * n + 16]

    def combine(i, d, slot):
        part_copy(i).wait_recv()
        mine, theirs = part_mine[slot, 1], part_recv[i, 1]
        top0, top1 = mine[:, 0:1], theirs[:, 0:1]
        top = jnp.maximum(top0, top1)
        factor0 = jnp.exp2((top0 - top) * FACTOR)
        factor1 = jnp.exp2((top1 - top) * FACTOR)
        total = factor0 * mine[:, 64:65] + factor1 * theirs[:, 64:65]
        out = (factor0 * part_mine[slot, 0] + factor1 * part_recv[i, 0]) / total
        out = out.astype(bf16)
        for n in range(4):
            att[slot, :, 128 * n : 128 * n + 128] = out[32 * n : 32 * n + 32]

        @pl.when((d == CHIPS - 1) & (c == 1))
        def _():
            decode_rows(slot)

    def project(slot, sub):
        return jnp.dot(att[slot], wbuf[:, lanes(sub, width)], preferred_element_type=f32)

    right, left = 2 * ((y + 1) % CHIPS) + c, 2 * ((y + 7) % CHIPS) + c

    def rs_copy(way, step, sub):
        return remote(
            rs_send.at[way, step, sub], rs_recv.at[way, step, sub],
            rs_ssem.at[way, step, sub], rs_rsem.at[way, step, sub], right if way == 0 else left,
        )

    far = (y + 4) % CHIPS
    attend_both(0, far, 0)
    locals_[8].wait()
    locals_[9].wait()
    pairs[5].wait_recv()
    combine(0, far, 0)
    for j in range(2):
        for way in range(2):
            sub = j + 2 * way
            rs_send[way, 0, sub] = project(0, sub).astype(bf16)
            rs_copy(way, 0, sub).start()

    def step_body(step, carry):
        away = 4 - step
        ahead, behind = (y + away) % CHIPS, (y + CHIPS - away) % CHIPS
        def both(j, carry):
            attend_both(2 * step - 1 + j, jnp.where(j == 0, ahead, behind), j)
            return carry
        lax.fori_loop(0, 2, both, 0)
        def join(j, carry):
            combine(2 * step - 1 + j, jnp.where(j == 0, ahead, behind), j)
            return carry
        lax.fori_loop(0, 2, join, 0)

        def sub_body(j, carry):
            for way in range(2):
                sub = (j + 2) % SUBS if way == 0 else j
                own = project(way, sub)

                @pl.when((step > 1) | (j >= 2))
                def _():
                    rs_copy(way, step - 1, sub).wait_recv()

                rs_send[way, step, sub] = (own + rs_recv[way, step - 1, sub].astype(f32)).astype(bf16)
                rs_copy(way, step, sub).start()
            return carry
        return lax.fori_loop(0, SUBS, sub_body, carry)

    lax.fori_loop(1, 4, step_body, 0)

    attend_both(7, y, 0)
    combine(7, y, 0)
    locals_[10].wait()
    locals_[11].wait()

    def own_body(sub, carry):
        hid[:, lanes(sub, width)] = project(0, sub) + resbuf[:, lanes(sub, width)].astype(f32)
        return carry
    lax.fori_loop(0, SUBS, own_body, 0)

    def last_body(j, squares):
        for way in range(2):
            sub = (j + 2) % SUBS if way == 0 else j
            rs_copy(way, 3, sub).wait_recv()
            hid[:, lanes(sub, width)] += rs_recv[way, 3, sub].astype(f32)
        return squares
    lax.fori_loop(0, SUBS, last_body, 0)

    hidden = hid[...]
    out_res[...] = hidden.astype(bf16)
    mean_square = jnp.sum(hidden * hidden, axis=1, keepdims=True) * (1.0 / hidden.shape[1])
    out_norm[...] = (hidden * lax.rsqrt(mean_square + 1e-05) * gainbuf[...]).astype(bf16)

    for copy in qd_copies + kv_copies + pairs:
        copy.wait_send()

    @pl.when(c != half)
    def _():
        qd_pair.wait_send()

    for j in range(4):
        @pl.when(jnp.logical_not((c == 1) & (y == 4 + j)))
        def _():
            dec_copies[j].wait_send()

    def part_done(i, carry):
        part_copy(i).wait_send()
        return carry
    lax.fori_loop(0, 8, part_done, 0)
    for j in range(2):
        for way in range(2):
            rs_copy(way, 0, j + 2 * way).wait_send()

    def rs_done(n, carry):
        for way in range(2):
            rs_copy(way, 1 + n // SUBS, n % SUBS).wait_send()
        return carry
    lax.fori_loop(0, 3 * SUBS, rs_done, 0)


def per_device(
    prompt_queries, prompt_entries, history_cache, decode_queries, decode_entries, decode_cache,
    decode_lengths, prompt_start, out_weight, residual, norm_gain,
):
    hbm = pl.BlockSpec(memory_space=pltpu.HBM)
    smem = pl.BlockSpec(memory_space=pltpu.SMEM)
    vmem = pl.BlockSpec(memory_space=pltpu.VMEM)
    span = history_cache.shape[1]
    tokens, width = residual.shape
    dma = pltpu.SemaphoreType.DMA
    shape = jax.ShapeDtypeStruct(residual.shape, residual.dtype)
    return pl.pallas_call(
        kernel,
        out_shape=(shape, shape),
        in_specs=[smem, smem] + [hbm] * 9,
        out_specs=(vmem, vmem),
        scratch_shapes=[
            pltpu.VMEM((2, span + 32, 512), bf16),
            pltpu.VMEM(prompt_entries.shape, bf16),
            pltpu.VMEM((2, CHIPS, span + 32, 128), bf16),
            pltpu.VMEM((4, 512, 128), bf16),
            pltpu.VMEM((2, 2, 16, 48, 256), bf16),
            pltpu.VMEM((8, 16, 256), bf16),
            pltpu.VMEM((512, width), bf16),
            pltpu.VMEM((tokens, width), bf16),
            pltpu.VMEM((1, width), f32),
            pltpu.VMEM((2, 16, 128), bf16),
            pltpu.VMEM((8, 2, 128, 128), f32),
            pltpu.VMEM((8, 2, 128, 128), f32),
            pltpu.VMEM((2, 2, 128, 128), f32),
            pltpu.VMEM((4, 2, 64, 128), bf16),
            pltpu.VMEM((CHIPS, 2, 64, 128), bf16),
            pltpu.VMEM((2, 32, 512), bf16),
            pltpu.VMEM((2, 4, SUBS, 32, width // SUBS), bf16),
            pltpu.VMEM((2, 4, SUBS, 32, width // SUBS), bf16),
            pltpu.VMEM((tokens, width), f32),
            dma((12,)), dma((8,)), dma((8,)), dma((8,)), dma((8,)), dma((6,)), dma((6,)),
            dma((8,)), dma((8,)), dma((4,)), dma((8,)), dma((2, 4, SUBS)), dma((2, 4, SUBS)),
        ],
        compiler_params=pltpu.CompilerParams(collective_id=0, has_side_effects=True),
    )(
        prompt_start, decode_lengths, prompt_queries, prompt_entries, history_cache, decode_queries,
        decode_entries, decode_cache, out_weight, residual, norm_gain.reshape(1, -1),
    )


def solution(mesh):
    placed = (
        P("rep", "tp"),
        P("rep", "tp", None),
        P("rep", "tp", None),
        P("rep", "tp"),
        P("rep", None, None),
        P("rep", None, "tp", None),
        P("rep"),
        P("rep"),
        P("tp", None),
        P("tp", "rep"),
        P(None),
    )
    return jax.shard_map(
        per_device, mesh=mesh, in_specs=placed, out_specs=(P("tp", "rep"), P("tp", "rep")),
        check_vma=False,
    )
```

```python
import jax
import jax.numpy as jnp
from jax import lax
from jax.experimental import pallas as pl
from jax.experimental.pallas import tpu as pltpu
from jax.sharding import PartitionSpec as P

HEAD_DIM = 128
CHIPS = 8
GROUP = 16
SUBS = 4
MESH = pl.DeviceIdType.MESH
LOWEST = -(2.0**100)
FACTOR = HEAD_DIM**-0.5 * 1.4426950408889634
NEVER = 1 << 20

f32 = jnp.float32
bf16 = jnp.bfloat16


def dot_t(a, b):
    return lax.dot_general(a, b, (((1,), (1,)), ((), ())), preferred_element_type=f32)


def iota(shape, dim):
    return lax.broadcasted_iota(jnp.int32, shape, dim)


def kernel(
    start_in, lengths_in, pq, pe, hist, dq, de, dc, w, res,
    hid,
    start_ref, lengths_ref, stage, pbuf, kv, qbuf, dbuf, qd, wbuf, resbuf, fresh,
    dec_send, dec_recv, att, own, rs_send, rs_recv,
    local_sem, qd_ssem, qd_rsem, kv_ssem, kv_rsem, pair_ssem, pair_rsem,
    dec_ssem, dec_rsem, rs_ssem, rs_rsem,
):
    t = lax.axis_index("tp")
    y = t // 2
    c = t % 2
    head = y // 2
    half = y // 4
    partner = 2 * y + 1 - c
    outward = 2 * (y % 2) - 1
    span = hist.shape[1]
    entries = pe.shape[0]
    rows = pq.shape[0]
    width = rs_send.shape[-1]

    def chip(steps):
        return (y + outward * steps + CHIPS) % CHIPS

    def local(src, dst, n):
        return pltpu.make_async_copy(src, dst, local_sem.at[n])

    def remote(src, dst, ssem, rsem, device):
        return pltpu.make_async_remote_copy(
            src_ref=src, dst_ref=dst, send_sem=ssem, recv_sem=rsem,
            device_id={"tp": device}, device_id_type=MESH,
        )

    def lanes(index, size):
        return pl.ds(pl.multiple_of(index * size, size), size)

    locals_ = [
        local(hist, stage.at[:, pl.ds(0, span), :], 0),
        local(pe, pbuf, 1),
        local(hist.at[:, :, lanes(head, 128)], kv.at[:, t, pl.ds(0, span), :], 2),
        local(dc.at[:, :, :, lanes(c, 256)], dbuf.at[c], 3),
    ]
    for i in range(2):
        columns = pl.ds(128 * i, 128)
        locals_.append(local(pq.at[:, columns], qbuf.at[2 * c + i, pl.ds(0, rows), :], 4 + i))
        locals_.append(local(dq.at[:, columns], qbuf.at[2 * c + i, pl.ds(rows, 16), :], 6 + i))
    locals_ += [
        local(de.at[:, :, lanes(head, 128)], fresh, 8),
        local(w, wbuf.at[pl.ds(pl.multiple_of(256 * c, 256), 256), :], 9),
        local(res, resbuf, 10),
        local(start_in, start_ref, 11),
        local(lengths_in, lengths_ref, 12),
    ]
    for copy in locals_:
        copy.start()

    barrier = pltpu.get_barrier_semaphore()
    for k in range(1, GROUP):
        pl.semaphore_signal(
            barrier, inc=1, device_id={"tp": (t + k) % GROUP}, device_id_type=MESH
        )

    locals_[0].wait()
    locals_[1].wait()
    for i in range(2):
        stage[i, span : span + 32, :] = jnp.concatenate(
            [pbuf[:, i, :], jnp.zeros((32 - entries, pbuf.shape[2]), bf16)], axis=0
        )
    for i in range(2):
        kv[i, t, span : span + 32, :] = stage[i, span : span + 32, lanes(head, 128)]
    rs_recv[0, 0, 2:4] = jnp.zeros((2, 32, width), bf16)
    rs_recv[1, 0, 0:2] = jnp.zeros((2, 32, width), bf16)
    pl.semaphore_wait(barrier, GROUP - 1)

    place = t - 8 * half
    qd_copies = []
    for k in range(1, CHIPS):
        copy = remote(dq, qd.at[place], qd_ssem.at[k], qd_rsem.at[place], 2 * ((y + k) % CHIPS) + half)
        copy.start()
        qd_copies.append(copy)
    qd_pair = remote(dq, qd.at[place], qd_ssem.at[0], qd_rsem.at[place], partner)
    qd_own = pltpu.make_async_copy(dq, qd.at[place], qd_rsem.at[place])

    @pl.when(c == half)
    def _():
        qd_own.start()

    @pl.when(c != half)
    def _():
        qd_pair.start()

    kv_copies = []

    def send_kv(src, slot, device):
        n = len(kv_copies)
        copy = remote(src, kv.at[:, slot], kv_ssem.at[n], kv_rsem.at[slot], device)
        copy.start()
        kv_copies.append(copy)

    def own_block(there):
        return stage.at[:, :, lanes(there // 2, 128)]

    mate = chip(-1)
    for steps in (3, -2, 1, -1):
        there = chip(steps)
        send_kv(own_block(there), t, 2 * there + c)

    pairs = [remote(dc.at[:, :, :, lanes(1 - c, 256)], dbuf.at[c], pair_ssem.at[0], pair_rsem.at[0], partner)]
    for i in range(2):
        columns = pl.ds(128 * i, 128)
        pairs.append(
            remote(pq.at[:, columns], qbuf.at[2 * c + i, pl.ds(0, rows), :],
                   pair_ssem.at[1 + i], pair_rsem.at[1 + i], partner)
        )
        pairs.append(
            remote(dq.at[:, columns], qbuf.at[2 * c + i, pl.ds(rows, 16), :],
                   pair_ssem.at[3 + i], pair_rsem.at[3 + i], partner)
        )
    pairs.append(
        remote(w, wbuf.at[pl.ds(pl.multiple_of(256 * c, 256), 256), :],
               pair_ssem.at[5], pair_rsem.at[5], partner)
    )
    for copy in pairs:
        copy.start()
    send_kv(own_block(y), t, partner)

    def wait_kv(slot):
        pltpu.make_async_copy(kv.at[:, slot], kv.at[:, slot], kv_rsem.at[slot]).wait()

    for steps in (2, 1, 3):
        slot = 2 * chip(steps) + c
        wait_kv(slot)
        send_kv(kv.at[:, slot], slot, 2 * mate + c)
        send_kv(kv.at[:, slot], slot, partner)

    locals_[11].wait()
    locals_[12].wait()
    row_b = iota((128, 1), 0) & 15
    limit = jnp.zeros((128, 1), jnp.int32)
    for b in range(16):
        limit = jnp.where(row_b == b, lengths_ref[b], limit)
    col = iota((1, 768), 1)
    col_b = (col * 1366) >> 16
    col_p = col - 48 * col_b
    lane = iota((128, 128), 1)

    locals_[3].wait()
    pairs[0].wait_recv()
    for s in range(8):
        pltpu.make_async_copy(dq, qd.at[s], qd_rsem.at[s]).wait()
    for g in range(2):
        columns = slice(128 * g, 128 * g + 128)
        q = jnp.concatenate(
            [qd[4 * g + n, :, 128 * i : 128 * i + 128] for n in range(4) for i in range(2)], axis=0
        )
        scores = []
        for core in range(2):
            keys = dbuf[core, 0, :, :, columns].reshape(768, 128)
            places = (2 * y + core) * 48 + col_p
            valid = (col_b == row_b) & (places < limit)
            scores.append(jnp.where(valid, dot_t(q, keys), LOWEST))
        top = jnp.maximum(*[jnp.max(s, axis=1, keepdims=True) for s in scores])
        top = top.astype(bf16).astype(f32)
        total = jnp.zeros((128, 1), f32)
        summed = jnp.zeros((128, 128), f32)
        for core in range(2):
            weights = jnp.exp2((scores[core] - top) * FACTOR)
            total += jnp.sum(weights, axis=1, keepdims=True)
            values = dbuf[core, 1, :, :, columns].reshape(768, 128)
            summed += jnp.dot(weights.astype(bf16), values, preferred_element_type=f32)
        stats = jnp.where(lane < 64, top, total).astype(bf16)
        summed = summed.astype(bf16)
        for n in range(2):
            dec_send[2 * g + n, 0] = summed[64 * n : 64 * n + 64]
            dec_send[2 * g + n, 1] = stats[64 * n : 64 * n + 64]
    dec_copies = []
    for j in range(4):
        copy = remote(dec_send.at[j], dec_recv.at[y], dec_ssem.at[j], dec_rsem.at[y], 2 * (4 * c + j) + 1)
        dec_copies.append(copy)
        stays = (c == 1) & (y == 4 + j)

        @pl.when(stays)
        def _():
            dec_recv[y] = dec_send[j]

        @pl.when(jnp.logical_not(stays))
        def _():
            copy.start()

    for steps in (-1, -3, -2, -4):
        slot = 2 * chip(steps) + c
        wait_kv(slot)
        send_kv(kv.at[:, slot], slot, partner)
    col = iota((1, 1536), 1)
    owner = (col * 683) >> 16
    place = col - 96 * owner
    start = start_ref[0]
    from_history = jnp.where(owner * span + place < start, -1, NEVER)
    from_prompt = jnp.where(place < span + entries, owner * entries + place - span, NEVER)
    first_row = jnp.where(place < span, from_history, from_prompt)
    row32 = iota((128, 1), 0) & 31

    for n in (2, 4, 5, 6, 7):
        locals_[n].wait()
    for copy in pairs[1:5]:
        copy.wait_recv()
    for k in range(CHIPS):
        wait_kv(2 * ((y + k) % CHIPS) + 1 - c)

    def decode_rows(slot):
        for s in range(CHIPS):
            @pl.when(jnp.logical_not((y == s) & (y >= 4)))
            def _():
                pltpu.make_async_copy(dec_send.at[0], dec_recv.at[s], dec_rsem.at[s]).wait()
        query = qbuf[:, rows : rows + 16, :].astype(f32)
        key = fresh[0].astype(f32)
        value = fresh[1].astype(f32)
        own = jnp.sum(query * key[None], axis=-1, keepdims=True).reshape(64, 1)
        value = jnp.concatenate([value] * 4, axis=0)
        tops = [dec_recv[s, 1, :, 0:1].astype(f32) for s in range(CHIPS)]
        top = own
        for s in range(CHIPS):
            top = jnp.maximum(top, tops[s])
        own_weight = jnp.exp2((own - top) * FACTOR)
        total = own_weight
        summed = own_weight.astype(bf16).astype(f32) * value
        for s in range(CHIPS):
            factor = jnp.exp2((tops[s] - top) * FACTOR)
            total += factor * dec_recv[s, 1, :, 64:65].astype(f32)
            summed += factor * dec_recv[s, 0].astype(f32)
        out = (summed / total).astype(bf16)
        for n in range(4):
            att[slot, 16:32, 128 * n : 128 * n + 128] = out[16 * n : 16 * n + 16]

    def attend(d, slot):
        row = pl.multiple_of(64 * d + 32 * c, 32)
        q = qbuf[:, pl.ds(row, 32), :].reshape(128, 128)
        keys = kv[0].reshape(1536, 128)
        values = kv[1].reshape(1536, 128)
        scores = jnp.where(first_row <= row + row32, dot_t(q, keys), LOWEST)
        top = jnp.max(scores, axis=1, keepdims=True)
        weights = jnp.exp2((scores - top) * FACTOR)
        total = jnp.sum(weights, axis=1, keepdims=True)
        summed = jnp.dot(weights.astype(bf16), values, preferred_element_type=f32)
        out = (summed / total).astype(bf16)
        for n in range(4):
            att[slot, :, 128 * n : 128 * n + 128] = out[32 * n : 32 * n + 32]

        @pl.when((d == CHIPS - 1) & (c == 1))
        def _():
            decode_rows(slot)

    def project(sub):
        return jnp.dot(att[0], wbuf[:, lanes(sub, width)], preferred_element_type=f32)

    right, left = 2 * ((y + 1) % CHIPS) + c, 2 * ((y + 7) % CHIPS) + c

    def rs_copy(way, step, sub):
        return remote(
            rs_send.at[way, step, sub], rs_recv.at[way, step, sub],
            rs_ssem.at[way, step, sub], rs_rsem.at[way, step, sub], right if way == 0 else left,
        )

    locals_[8].wait()
    attend((y + 4) % CHIPS, 0)
    locals_[9].wait()
    pairs[5].wait_recv()

    def first_body(j, carry):
        for way in range(2):
            sub = j + 2 * way
            rs_send[way, 0, sub] = project(sub).astype(bf16)
            rs_copy(way, 0, sub).start()
        return carry
    lax.fori_loop(0, 2, first_body, 0)

    def step_body(step, carry):
        away = 4 - step

        def attend_body(j, carry):
            attend((y + CHIPS + away * (1 - 2 * j)) % CHIPS, j)
            return carry
        lax.fori_loop(0, 2, attend_body, 0)

        def own_body(sub, carry):
            both = att[...].reshape(64, 512)
            own[sub] = jnp.dot(both, wbuf[:, lanes(sub, width)], preferred_element_type=f32)
            return carry
        lax.fori_loop(0, SUBS, own_body, 0)

        def sub_body(j, carry):
            for way in range(2):
                sub = (j + 2) % SUBS if way == 0 else j

                @pl.when((step > 1) | (j >= 2))
                def _():
                    rs_copy(way, step - 1, sub).wait_recv()

                added = own[sub, 32 * way : 32 * way + 32] + rs_recv[way, step - 1, sub].astype(f32)
                rs_send[way, step, sub] = added.astype(bf16)
                rs_copy(way, step, sub).start()
            return carry
        return lax.fori_loop(0, SUBS, sub_body, carry)

    lax.fori_loop(1, 4, step_body, 0)

    attend(y, 0)
    locals_[10].wait()

    def mine_body(sub, carry):
        hid[:, lanes(sub, width)] = project(sub) + resbuf[:, lanes(sub, width)].astype(f32)
        return carry
    lax.fori_loop(0, SUBS, mine_body, 0)

    def last_body(j, carry):
        for way in range(2):
            sub = (j + 2) % SUBS if way == 0 else j
            rs_copy(way, 3, sub).wait_recv()
            hid[:, lanes(sub, width)] += rs_recv[way, 3, sub].astype(f32)
        return carry
    lax.fori_loop(0, SUBS, last_body, 0)

    for copy in qd_copies + kv_copies + pairs:
        copy.wait_send()

    @pl.when(c != half)
    def _():
        qd_pair.wait_send()

    for j in range(4):
        @pl.when(jnp.logical_not((c == 1) & (y == 4 + j)))
        def _():
            dec_copies[j].wait_send()

    for j in range(2):
        for way in range(2):
            rs_copy(way, 0, j + 2 * way).wait_send()

    def rs_done(n, carry):
        for way in range(2):
            rs_copy(way, 1 + n // SUBS, n % SUBS).wait_send()
        return carry
    lax.fori_loop(0, 3 * SUBS, rs_done, 0)


def finish(hid, gain, out_res, out_norm):
    hidden = hid[...]
    out_res[...] = hidden.astype(bf16)
    mean_square = jnp.sum(hidden * hidden, axis=1, keepdims=True) * (1.0 / hidden.shape[1])
    out_norm[...] = (hidden * lax.rsqrt(mean_square + 1e-05) * gain[...]).astype(bf16)


def per_device(
    prompt_queries, prompt_entries, history_cache, decode_queries, decode_entries, decode_cache,
    decode_lengths, prompt_start, out_weight, residual, norm_gain,
):
    hbm = pl.BlockSpec(memory_space=pltpu.HBM)
    vmem = pl.BlockSpec(memory_space=pltpu.VMEM)
    span = history_cache.shape[1]
    entries = prompt_entries.shape[1]
    tokens, width = residual.shape
    dma = pltpu.SemaphoreType.DMA
    hidden = pl.pallas_call(
        kernel,
        out_shape=jax.ShapeDtypeStruct((tokens, width), f32),
        in_specs=[hbm] * 10,
        out_specs=vmem,
        scratch_shapes=[
            pltpu.SMEM(prompt_start.shape, jnp.int32),
            pltpu.SMEM(decode_lengths.shape, jnp.int32),
            pltpu.VMEM((2, span + 32, 512), bf16),
            pltpu.VMEM((entries, 2, 512), bf16),
            pltpu.VMEM((2, GROUP, span + 32, 128), bf16),
            pltpu.VMEM((4, 512, 128), bf16),
            pltpu.VMEM((2, 2, 16, 48, 256), bf16),
            pltpu.VMEM((8, 16, 256), bf16),
            pltpu.VMEM((512, width), bf16),
            pltpu.VMEM((tokens, width), bf16),
            pltpu.VMEM((2, 16, 128), bf16),
            pltpu.VMEM((4, 2, 64, 128), bf16),
            pltpu.VMEM((CHIPS, 2, 64, 128), bf16),
            pltpu.VMEM((2, 32, 512), bf16),
            pltpu.VMEM((SUBS, 64, width // SUBS), f32),
            pltpu.VMEM((2, 4, SUBS, 32, width // SUBS), bf16),
            pltpu.VMEM((2, 4, SUBS, 32, width // SUBS), bf16),
            dma((13,)), dma((8,)), dma((8,)), dma((16,)), dma((16,)), dma((6,)), dma((6,)),
            dma((4,)), dma((8,)), dma((2, 4, SUBS)), dma((2, 4, SUBS)),
        ],
        compiler_params=pltpu.CompilerParams(collective_id=0, has_side_effects=True),
    )(
        prompt_start, decode_lengths, prompt_queries, prompt_entries.transpose(1, 0, 2), history_cache,
        decode_queries, decode_entries, decode_cache, out_weight, residual,
    )
    shape = jax.ShapeDtypeStruct(residual.shape, residual.dtype)
    return pl.pallas_call(
        finish, out_shape=(shape, shape), in_specs=[vmem, vmem], out_specs=(vmem, vmem),
    )(hidden, norm_gain.reshape(1, -1))


def solution(mesh):
    placed = (
        P("rep", "tp"),
        P("rep", "tp", None),
        P("rep", "tp", None),
        P("rep", "tp"),
        P("rep", None, None),
        P("rep", None, "tp", None),
        P("rep"),
        P("rep"),
        P("tp", None),
        P("tp", "rep"),
        P(None),
    )
    return jax.shard_map(
        per_device, mesh=mesh, in_specs=placed, out_specs=(P("tp", "rep"), P("tp", "rep")),
        check_vma=False,
    )
```

```python
import jax
import jax.numpy as jnp
from jax import lax
from jax.experimental import pallas as pl
from jax.experimental.pallas import tpu as pltpu
from jax.sharding import PartitionSpec as P

HEAD_DIM = 128
CHIPS = 8
GROUP = 16
SUBS = 2
HALF = SUBS // 2
MESH = pl.DeviceIdType.MESH
LOWEST = -(2.0**100)
FACTOR = HEAD_DIM**-0.5 * 1.4426950408889634
NEVER = 1 << 20

f32 = jnp.float32
bf16 = jnp.bfloat16


def dot_t(a, b):
    return lax.dot_general(a, b, (((1,), (1,)), ((), ())), preferred_element_type=f32)


def iota(shape, dim):
    return lax.broadcasted_iota(jnp.int32, shape, dim)


def kernel(
    start_in, lengths_in, pq, pe, hist, dq, de, dc, w, res,
    hid,
    start_ref, lengths_ref, stage, pbuf, kv, qbuf, dbuf, qd, wbuf, resbuf, fresh,
    dec_send, dec_recv, att, own, rs_send, rs_recv,
    local_sem, qd_ssem, qd_rsem, kv_ssem, kv_rsem, pair_ssem, pair_rsem,
    dec_ssem, dec_rsem, rs_ssem, rs_rsem, plane_sem,
):
    t = lax.axis_index("tp")
    y = t // 2
    c = t % 2
    head = y // 2
    half = y // 4
    partner = 2 * y + 1 - c
    outward = 2 * (y % 2) - 1
    span = hist.shape[1]
    entries = pe.shape[0]
    rows = pq.shape[0]
    width = rs_send.shape[-1]

    def chip(steps):
        return (y + outward * steps + CHIPS) % CHIPS

    def local(src, dst, n):
        return pltpu.make_async_copy(src, dst, local_sem.at[n])

    def remote(src, dst, ssem, rsem, device):
        return pltpu.make_async_remote_copy(
            src_ref=src, dst_ref=dst, send_sem=ssem, recv_sem=rsem,
            device_id={"tp": device}, device_id_type=MESH,
        )

    def lanes(index, size):
        return pl.ds(pl.multiple_of(index * size, size), size)

    locals_ = [
        local(start_in, start_ref, 0),
        local(pe, pbuf, 1),
        local(hist.at[:, :, lanes(head, 128)], kv.at[t, :, pl.ds(0, span), :], 2),
        local(dc.at[:, :, :, lanes(c, 256)], dbuf.at[c], 3),
    ]
    for i in range(2):
        columns = pl.ds(128 * i, 128)
        locals_.append(local(pq.at[:, columns], qbuf.at[2 * c + i, pl.ds(0, rows), :], 4 + i))
        locals_.append(local(dq.at[:, columns], qbuf.at[2 * c + i, pl.ds(rows, 16), :], 6 + i))
    locals_ += [
        local(de.at[:, :, lanes(head, 128)], fresh, 8),
        local(w.at[:, pl.ds(0, width)], wbuf.at[0, pl.ds(pl.multiple_of(256 * c, 256), 256), :], 9),
        local(res, resbuf, 10),
        local(lengths_in, lengths_ref, 11),
    ]
    own_weights = [locals_[9]] + [
        local(w.at[:, pl.ds(sub * width, width)], wbuf.at[sub, pl.ds(pl.multiple_of(256 * c, 256), 256), :], 15 + sub)
        for sub in range(1, SUBS)
    ]
    staged = [
        local(hist.at[:, :, pl.ds(128 * h, 128)], stage.at[h, :, pl.ds(0, span), :], 12 + h)
        for h in range(4)
    ]
    for copy in [locals_[1]] + staged + locals_[:1] + locals_[2:] + own_weights[1:]:
        copy.start()

    barrier = pltpu.get_barrier_semaphore()
    for k in range(1, CHIPS):
        pl.semaphore_signal(
            barrier, inc=1, device_id={"tp": 2 * ((y + k) % CHIPS) + c}, device_id_type=MESH
        )
    pl.semaphore_signal(barrier, inc=1, device_id={"tp": partner}, device_id_type=MESH)

    locals_[1].wait()
    for i in range(2):
        block = jnp.concatenate(
            [pbuf[:, i, :], jnp.zeros((32 - entries, pbuf.shape[2]), bf16)], axis=0
        )
        for h in range(4):
            stage[h, i, span : span + 32, :] = block[:, 128 * h : 128 * h + 128]
    for i in range(2):
        kv[t, i, span : span + 32, :] = stage[head, i, span : span + 32, :]
    for copy in staged:
        copy.wait()
    rs_recv[0, 0, HALF:] = jnp.zeros((HALF, 32, width), bf16)
    rs_recv[1, 0, :HALF] = jnp.zeros((HALF, 32, width), bf16)
    pl.semaphore_wait(barrier, CHIPS)
    pl.semaphore_signal(plane_sem, inc=1, device_id={"tp": partner}, device_id_type=MESH)

    kv_copies = []

    def send_kv(src, slot, device):
        n = len(kv_copies)
        copy = remote(src, kv.at[slot], kv_ssem.at[n], kv_rsem.at[slot], device)
        copy.start()
        kv_copies.append(copy)

    def own_block(there):
        return stage.at[there // 2]

    mate = chip(-1)
    for steps in (3, -3, 2, -2, 1, -1):
        there = chip(steps)
        send_kv(own_block(there), t, 2 * there + c)

    pairs = [remote(dc.at[:, :, :, lanes(1 - c, 256)], dbuf.at[c], pair_ssem.at[0], pair_rsem.at[0], partner)]
    for i in range(2):
        columns = pl.ds(128 * i, 128)
        pairs.append(
            remote(pq.at[:, columns], qbuf.at[2 * c + i, pl.ds(0, rows), :],
                   pair_ssem.at[1 + i], pair_rsem.at[1 + i], partner)
        )
        pairs.append(
            remote(dq.at[:, columns], qbuf.at[2 * c + i, pl.ds(rows, 16), :],
                   pair_ssem.at[3 + i], pair_rsem.at[3 + i], partner)
        )
    for sub in range(SUBS):
        pairs.append(
            remote(w.at[:, pl.ds(sub * width, width)], wbuf.at[sub, pl.ds(pl.multiple_of(256 * c, 256), 256), :],
                   pair_ssem.at[5 + sub], pair_rsem.at[5 + sub], partner)
        )
    weights_in = pairs[5:]
    for copy in pairs[:5]:
        copy.start()
    pl.semaphore_wait(plane_sem, 1)

    place = t - 8 * half
    qd_copies = []
    for k in range(1, CHIPS):
        copy = remote(dq, qd.at[place], qd_ssem.at[k], qd_rsem.at[place], 2 * ((y + k) % CHIPS) + half)
        copy.start()
        qd_copies.append(copy)
    qd_pair = remote(dq, qd.at[place], qd_ssem.at[0], qd_rsem.at[place], partner)
    qd_own = pltpu.make_async_copy(dq, qd.at[place], qd_rsem.at[place])

    @pl.when(c == half)
    def _():
        qd_own.start()

    @pl.when(c != half)
    def _():
        qd_pair.start()

    send_kv(own_block(y), t, partner)
    order = [n + HALF * way for n in range(HALF) for way in range(2)]
    for n in order[:HALF]:
        weights_in[n].start()

    def wait_kv(slot):
        pltpu.make_async_copy(kv.at[slot], kv.at[slot], kv_rsem.at[slot]).wait()

    def take_kv(steps):
        slot = 2 * chip(steps) + c
        wait_kv(slot)
        if steps == 3:
            send_kv(kv.at[slot], slot, 2 * mate + c)
        send_kv(kv.at[slot], slot, partner)

    take_kv(3)
    take_kv(-3)
    for n in order[HALF:]:
        weights_in[n].start()
    take_kv(2)
    take_kv(-2)

    locals_[11].wait()
    row_b = iota((128, 1), 0) & 15
    limit = jnp.zeros((128, 1), jnp.int32)
    for b in range(16):
        limit = jnp.where(row_b == b, lengths_ref[b], limit)
    col = iota((1, 768), 1)
    col_b = (col * 1366) >> 16
    col_p = col - 48 * col_b
    lane = iota((128, 128), 1)

    locals_[3].wait()
    pairs[0].wait_recv()
    for s in range(8):
        pltpu.make_async_copy(dq, qd.at[s], qd_rsem.at[s]).wait()
    for g in range(2):
        columns = slice(128 * g, 128 * g + 128)
        q = jnp.concatenate(
            [qd[4 * g + n, :, 128 * i : 128 * i + 128] for n in range(4) for i in range(2)], axis=0
        )
        scores = []
        for core in range(2):
            keys = dbuf[core, 0, :, :, columns].reshape(768, 128)
            places = (2 * y + core) * 48 + col_p
            valid = (col_b == row_b) & (places < limit)
            scores.append(jnp.where(valid, dot_t(q, keys), LOWEST))
        top = jnp.maximum(*[jnp.max(s, axis=1, keepdims=True) for s in scores])
        top = top.astype(bf16).astype(f32)
        total = jnp.zeros((128, 1), f32)
        summed = jnp.zeros((128, 128), f32)
        for core in range(2):
            weights = jnp.exp2((scores[core] - top) * FACTOR)
            total += jnp.sum(weights, axis=1, keepdims=True)
            values = dbuf[core, 1, :, :, columns].reshape(768, 128)
            summed += jnp.dot(weights.astype(bf16), values, preferred_element_type=f32)
        stats = jnp.where(lane < 64, top, total).astype(bf16)
        summed = summed.astype(bf16)
        for n in range(2):
            dec_send[2 * g + n, 0] = summed[64 * n : 64 * n + 64]
            dec_send[2 * g + n, 1] = stats[64 * n : 64 * n + 64]
    dec_copies = []
    for j in range(4):
        copy = remote(dec_send.at[j], dec_recv.at[y], dec_ssem.at[j], dec_rsem.at[y], 2 * (4 * c + j) + 1)
        dec_copies.append(copy)
        stays = (c == 1) & (y == 4 + j)

        @pl.when(stays)
        def _():
            dec_recv[y] = dec_send[j]

        @pl.when(jnp.logical_not(stays))
        def _():
            copy.start()

    for steps in (1, -1, -4):
        take_kv(steps)
    col = iota((1, 1536), 1)
    owner = (col * 683) >> 16
    place = col - 96 * owner
    locals_[0].wait()
    start = start_ref[0]
    from_history = jnp.where(owner * span + place < start, -1, NEVER)
    from_prompt = jnp.where(place < span + entries, owner * entries + place - span, NEVER)
    first_row = jnp.where(place < span, from_history, from_prompt)
    row32 = iota((128, 1), 0) & 31

    for n in (2, 4, 5, 6, 7):
        locals_[n].wait()
    for copy in pairs[1:5]:
        copy.wait_recv()
    for k in range(CHIPS):
        wait_kv(2 * ((y + k) % CHIPS) + 1 - c)

    def decode_rows(slot):
        for s in range(CHIPS):
            @pl.when(jnp.logical_not((y == s) & (y >= 4)))
            def _():
                pltpu.make_async_copy(dec_send.at[0], dec_recv.at[s], dec_rsem.at[s]).wait()
        query = qbuf[:, rows : rows + 16, :].astype(f32)
        key = fresh[0].astype(f32)
        value = fresh[1].astype(f32)
        own = jnp.sum(query * key[None], axis=-1, keepdims=True).reshape(64, 1)
        value = jnp.concatenate([value] * 4, axis=0)
        tops = [dec_recv[s, 1, :, 0:1].astype(f32) for s in range(CHIPS)]
        top = own
        for s in range(CHIPS):
            top = jnp.maximum(top, tops[s])
        own_weight = jnp.exp2((own - top) * FACTOR)
        total = own_weight
        summed = own_weight.astype(bf16).astype(f32) * value
        for s in range(CHIPS):
            factor = jnp.exp2((tops[s] - top) * FACTOR)
            total += factor * dec_recv[s, 1, :, 64:65].astype(f32)
            summed += factor * dec_recv[s, 0].astype(f32)
        out = (summed / total).astype(bf16)
        for n in range(4):
            att[slot, 16:32, 128 * n : 128 * n + 128] = out[16 * n : 16 * n + 16]

    def attend(d, slot):
        row = pl.multiple_of(64 * d + 32 * c, 32)
        q = qbuf[:, pl.ds(row, 32), :].reshape(128, 128)
        keys = kv[:, 0].reshape(1536, 128)
        values = kv[:, 1].reshape(1536, 128)
        scores = jnp.where(first_row <= row + row32, dot_t(q, keys), LOWEST)
        top = jnp.max(scores, axis=1, keepdims=True)
        weights = jnp.exp2((scores - top) * FACTOR)
        total = jnp.sum(weights, axis=1, keepdims=True)
        summed = jnp.dot(weights.astype(bf16), values, preferred_element_type=f32)
        out = (summed / total).astype(bf16)
        for n in range(4):
            att[slot, :, 128 * n : 128 * n + 128] = out[32 * n : 32 * n + 32]

        @pl.when((d == CHIPS - 1) & (c == 1))
        def _():
            decode_rows(slot)

    def project(sub):
        return jnp.dot(att[0], wbuf[sub], preferred_element_type=f32)

    right, left = 2 * ((y + 1) % CHIPS) + c, 2 * ((y + 7) % CHIPS) + c

    def rs_copy(way, step, sub):
        return remote(
            rs_send.at[way, step, sub], rs_recv.at[way, step, sub],
            rs_ssem.at[way, step, sub], rs_rsem.at[way, step, sub], right if way == 0 else left,
        )

    locals_[8].wait()
    attend((y + 4) % CHIPS, 0)
    for copy in own_weights:
        copy.wait()
    for copy in weights_in:
        copy.wait_recv()

    def first_body(j, carry):
        for way in range(2):
            sub = j + HALF * way
            rs_send[way, 0, sub] = project(sub).astype(bf16)
            rs_copy(way, 0, sub).start()
        return carry
    lax.fori_loop(0, HALF, first_body, 0)

    def step_body(step, carry):
        away = 4 - step

        def attend_body(j, carry):
            attend((y + CHIPS + away * (1 - 2 * j)) % CHIPS, j)
            return carry
        lax.fori_loop(0, 2, attend_body, 0)

        def own_body(sub, carry):
            both = att[...].reshape(64, 512)
            own[sub] = jnp.dot(both, wbuf[sub], preferred_element_type=f32)
            return carry
        lax.fori_loop(0, SUBS, own_body, 0)

        def sub_body(j, carry):
            for way in range(2):
                sub = (j + HALF) % SUBS if way == 0 else j

                @pl.when((step > 1) | (j >= HALF))
                def _():
                    rs_copy(way, step - 1, sub).wait_recv()

                added = own[sub, 32 * way : 32 * way + 32] + rs_recv[way, step - 1, sub].astype(f32)
                rs_send[way, step, sub] = added.astype(bf16)
                rs_copy(way, step, sub).start()
            return carry
        return lax.fori_loop(0, SUBS, sub_body, carry)

    lax.fori_loop(1, 4, step_body, 0)

    attend(y, 0)
    locals_[10].wait()

    def mine_body(sub, carry):
        hid[:, lanes(sub, width)] = project(sub) + resbuf[:, lanes(sub, width)].astype(f32)
        return carry
    lax.fori_loop(0, SUBS, mine_body, 0)

    def last_body(j, carry):
        for way in range(2):
            sub = (j + HALF) % SUBS if way == 0 else j
            rs_copy(way, 3, sub).wait_recv()
            hid[:, lanes(sub, width)] += rs_recv[way, 3, sub].astype(f32)
        return carry
    lax.fori_loop(0, SUBS, last_body, 0)

    for copy in qd_copies + kv_copies + pairs:
        copy.wait_send()

    @pl.when(c != half)
    def _():
        qd_pair.wait_send()

    for j in range(4):
        @pl.when(jnp.logical_not((c == 1) & (y == 4 + j)))
        def _():
            dec_copies[j].wait_send()

    for j in range(HALF):
        for way in range(2):
            rs_copy(way, 0, j + HALF * way).wait_send()

    def rs_done(n, carry):
        for way in range(2):
            rs_copy(way, 1 + n // SUBS, n % SUBS).wait_send()
        return carry
    lax.fori_loop(0, 3 * SUBS, rs_done, 0)


def finish(hid, gain, out_res, out_norm):
    hidden = hid[...]
    out_res[...] = hidden.astype(bf16)
    mean_square = jnp.sum(hidden * hidden, axis=1, keepdims=True) * (1.0 / hidden.shape[1])
    out_norm[...] = (hidden * lax.rsqrt(mean_square + 1e-05) * gain[...]).astype(bf16)


def per_device(
    prompt_queries, prompt_entries, history_cache, decode_queries, decode_entries, decode_cache,
    decode_lengths, prompt_start, out_weight, residual, norm_gain,
):
    hbm = pl.BlockSpec(memory_space=pltpu.HBM)
    vmem = pl.BlockSpec(memory_space=pltpu.VMEM)
    span = history_cache.shape[1]
    entries = prompt_entries.shape[1]
    tokens, width = residual.shape
    dma = pltpu.SemaphoreType.DMA
    hidden = pl.pallas_call(
        kernel,
        out_shape=jax.ShapeDtypeStruct((tokens, width), f32),
        in_specs=[hbm] * 10,
        out_specs=vmem,
        scratch_shapes=[
            pltpu.SMEM(prompt_start.shape, jnp.int32),
            pltpu.SMEM(decode_lengths.shape, jnp.int32),
            pltpu.VMEM((4, 2, span + 32, 128), bf16),
            pltpu.VMEM((entries, 2, 512), bf16),
            pltpu.VMEM((GROUP, 2, span + 32, 128), bf16),
            pltpu.VMEM((4, 512, 128), bf16),
            pltpu.VMEM((2, 2, 16, 48, 256), bf16),
            pltpu.VMEM((8, 16, 256), bf16),
            pltpu.VMEM((SUBS, 512, width // SUBS), bf16),
            pltpu.VMEM((tokens, width), bf16),
            pltpu.VMEM((2, 16, 128), bf16),
            pltpu.VMEM((4, 2, 64, 128), bf16),
            pltpu.VMEM((CHIPS, 2, 64, 128), bf16),
            pltpu.VMEM((2, 32, 512), bf16),
            pltpu.VMEM((SUBS, 64, width // SUBS), f32),
            pltpu.VMEM((2, 4, SUBS, 32, width // SUBS), bf16),
            pltpu.VMEM((2, 4, SUBS, 32, width // SUBS), bf16),
            dma((15 + SUBS,)), dma((8,)), dma((8,)), dma((16,)), dma((16,)), dma((5 + SUBS,)), dma((5 + SUBS,)),
            dma((4,)), dma((8,)), dma((2, 4, SUBS)), dma((2, 4, SUBS)), pltpu.SemaphoreType.REGULAR,
        ],
        compiler_params=pltpu.CompilerParams(collective_id=0, has_side_effects=True),
    )(
        prompt_start, decode_lengths, prompt_queries, prompt_entries.transpose(1, 0, 2), history_cache,
        decode_queries, decode_entries, decode_cache, out_weight, residual,
    )
    shape = jax.ShapeDtypeStruct(residual.shape, residual.dtype)
    return pl.pallas_call(
        finish, out_shape=(shape, shape), in_specs=[vmem, vmem], out_specs=(vmem, vmem),
    )(hidden, norm_gain.reshape(1, -1))


def solution(mesh):
    placed = (
        P("rep", "tp"),
        P("rep", "tp", None),
        P("rep", "tp", None),
        P("rep", "tp"),
        P("rep", None, None),
        P("rep", None, "tp", None),
        P("rep"),
        P("rep"),
        P("tp", None),
        P("tp", "rep"),
        P(None),
    )
    return jax.shard_map(
        per_device, mesh=mesh, in_specs=placed, out_specs=(P("tp", "rep"), P("tp", "rep")),
        check_vma=False,
    )
```

```python
import jax
import jax.numpy as jnp
from jax import lax
from jax.experimental import pallas as pl
from jax.experimental.pallas import tpu as pltpu
from jax.sharding import PartitionSpec as P

HEAD_DIM = 128
CHIPS = 8
GROUP = 16
SUBS = 2
HALF = SUBS // 2
MESH = pl.DeviceIdType.MESH
LOWEST = -(2.0**100)
FACTOR = HEAD_DIM**-0.5 * 1.4426950408889634
NEVER = 1 << 20

f32 = jnp.float32
bf16 = jnp.bfloat16


def dot_t(a, b):
    return lax.dot_general(a, b, (((1,), (1,)), ((), ())), preferred_element_type=f32)


def iota(shape, dim):
    return lax.broadcasted_iota(jnp.int32, shape, dim)


def kernel(
    start_in, lengths_in, pq, pe, hist, dq, de, dc, w, res,
    hid,
    start_ref, lengths_ref, stage, pbuf, kv, qbuf, dbuf, qd, wbuf, resbuf, fresh,
    dec_send, dec_recv, att, own, rs_send, rs_recv,
    local_sem, qd_ssem, qd_rsem, kv_ssem, kv_rsem, pair_ssem, pair_rsem,
    dec_ssem, dec_rsem, rs_ssem, rs_rsem, plane_sem,
):
    t = lax.axis_index("tp")
    y = t // 2
    c = t % 2
    head = y // 2
    half = y // 4
    partner = 2 * y + 1 - c
    outward = 2 * (y % 2) - 1
    span = hist.shape[1]
    entries = pe.shape[0]
    rows = pq.shape[0]
    width = rs_send.shape[-1]

    def chip(steps):
        return (y + outward * steps + CHIPS) % CHIPS

    def local(src, dst, n):
        return pltpu.make_async_copy(src, dst, local_sem.at[n])

    def remote(src, dst, ssem, rsem, device):
        return pltpu.make_async_remote_copy(
            src_ref=src, dst_ref=dst, send_sem=ssem, recv_sem=rsem,
            device_id={"tp": device}, device_id_type=MESH,
        )

    def lanes(index, size):
        return pl.ds(pl.multiple_of(index * size, size), size)

    locals_ = [
        local(start_in, start_ref, 0),
        local(pe, pbuf, 1),
        local(hist.at[:, :, lanes(head, 128)], kv.at[t, :, pl.ds(0, span), :], 2),
        local(dc.at[:, :, :, lanes(c, 256)], dbuf.at[c], 3),
    ]
    for i in range(2):
        columns = pl.ds(128 * i, 128)
        locals_.append(local(pq.at[:, columns], qbuf.at[2 * c + i, pl.ds(0, rows), :], 4 + i))
        locals_.append(local(dq.at[:, columns], qbuf.at[2 * c + i, pl.ds(rows, 16), :], 6 + i))
    locals_ += [
        local(de.at[:, :, lanes(head, 128)], fresh, 8),
        local(w.at[:, pl.ds(0, width)], wbuf.at[0, pl.ds(pl.multiple_of(256 * c, 256), 256), :], 9),
        local(res, resbuf, 10),
        local(lengths_in, lengths_ref, 11),
    ]
    own_weights = [locals_[9]] + [
        local(w.at[:, pl.ds(sub * width, width)], wbuf.at[sub, pl.ds(pl.multiple_of(256 * c, 256), 256), :], 15 + sub)
        for sub in range(1, SUBS)
    ]
    staged = [
        local(hist.at[:, :, pl.ds(128 * h, 128)], stage.at[h, :, pl.ds(0, span), :], 12 + h)
        for h in range(4)
    ]
    for copy in [locals_[1]] + staged + locals_[:1] + locals_[2:] + own_weights[1:]:
        copy.start()

    barrier = pltpu.get_barrier_semaphore()
    for k in range(1, CHIPS):
        pl.semaphore_signal(
            barrier, inc=1, device_id={"tp": 2 * ((y + k) % CHIPS) + c}, device_id_type=MESH
        )
    pl.semaphore_signal(barrier, inc=1, device_id={"tp": partner}, device_id_type=MESH)

    locals_[1].wait()
    for i in range(2):
        block = jnp.concatenate(
            [pbuf[:, i, :], jnp.zeros((32 - entries, pbuf.shape[2]), bf16)], axis=0
        )
        for h in range(4):
            stage[h, i, span : span + 32, :] = block[:, 128 * h : 128 * h + 128]
    for i in range(2):
        kv[t, i, span : span + 32, :] = stage[head, i, span : span + 32, :]
    for copy in staged:
        copy.wait()
    rs_recv[0, 0, HALF:] = jnp.zeros((HALF, 32, width), bf16)
    rs_recv[1, 0, :HALF] = jnp.zeros((HALF, 32, width), bf16)
    pl.semaphore_wait(barrier, CHIPS)
    pl.semaphore_signal(plane_sem, inc=1, device_id={"tp": partner}, device_id_type=MESH)

    place = t - 8 * half
    qd_copies = []
    for k in range(1, CHIPS):
        copy = remote(dq, qd.at[place], qd_ssem.at[k], qd_rsem.at[place], 2 * ((y + k) % CHIPS) + half)
        qd_copies.append(copy)

    def send_queries():
        for copy in qd_copies:
            copy.start()

    qd_pair = remote(dq, qd.at[place], qd_ssem.at[0], qd_rsem.at[place], partner)
    qd_own = pltpu.make_async_copy(dq, qd.at[place], qd_rsem.at[place])

    @pl.when(c == half)
    def _():
        qd_own.start()

    @pl.when(c != half)
    def _():
        qd_pair.start()

    @pl.when(c == half)
    def _():
        send_queries()

    kv_copies = []

    def send_kv(src, slot, device):
        n = len(kv_copies)
        copy = remote(src, kv.at[slot], kv_ssem.at[n], kv_rsem.at[slot], device)
        copy.start()
        kv_copies.append(copy)

    def own_block(there):
        return stage.at[there // 2]

    mate = chip(-1)
    for steps in (3, -3, 2, -2, 1, -1):
        there = chip(steps)
        send_kv(own_block(there), t, 2 * there + c)

    pairs = [remote(dc.at[:, :, :, lanes(1 - c, 256)], dbuf.at[c], pair_ssem.at[0], pair_rsem.at[0], partner)]
    for i in range(2):
        columns = pl.ds(128 * i, 128)
        pairs.append(
            remote(pq.at[:, columns], qbuf.at[2 * c + i, pl.ds(0, rows), :],
                   pair_ssem.at[1 + i], pair_rsem.at[1 + i], partner)
        )
        pairs.append(
            remote(dq.at[:, columns], qbuf.at[2 * c + i, pl.ds(rows, 16), :],
                   pair_ssem.at[3 + i], pair_rsem.at[3 + i], partner)
        )
    for sub in range(SUBS):
        pairs.append(
            remote(w.at[:, pl.ds(sub * width, width)], wbuf.at[sub, pl.ds(pl.multiple_of(256 * c, 256), 256), :],
                   pair_ssem.at[5 + sub], pair_rsem.at[5 + sub], partner)
        )
    weights_in = pairs[5:]
    for copy in pairs[:5]:
        copy.start()
    pl.semaphore_wait(plane_sem, 1)

    @pl.when(c != half)
    def _():
        send_queries()

    send_kv(own_block(y), t, partner)
    order = [n + HALF * way for n in range(HALF) for way in range(2)]
    for n in order[:HALF]:
        weights_in[n].start()

    def wait_kv(slot):
        pltpu.make_async_copy(kv.at[slot], kv.at[slot], kv_rsem.at[slot]).wait()

    def take_kv(steps):
        slot = 2 * chip(steps) + c
        wait_kv(slot)
        if steps == 3:
            send_kv(kv.at[slot], slot, 2 * mate + c)
        send_kv(kv.at[slot], slot, partner)

    take_kv(3)
    take_kv(-3)
    for n in order[HALF:]:
        weights_in[n].start()
    take_kv(2)
    take_kv(-2)

    locals_[11].wait()
    row_b = iota((128, 1), 0) & 15
    limit = jnp.zeros((128, 1), jnp.int32)
    for b in range(16):
        limit = jnp.where(row_b == b, lengths_ref[b], limit)
    col = iota((1, 768), 1)
    col_b = (col * 1366) >> 16
    col_p = col - 48 * col_b
    lane = iota((128, 128), 1)

    locals_[3].wait()
    pairs[0].wait_recv()
    for s in range(8):
        pltpu.make_async_copy(dq, qd.at[s], qd_rsem.at[s]).wait()
    for g in range(2):
        columns = slice(128 * g, 128 * g + 128)
        q = jnp.concatenate(
            [qd[4 * g + n, :, 128 * i : 128 * i + 128] for n in range(4) for i in range(2)], axis=0
        )
        scores = []
        for core in range(2):
            keys = dbuf[core, 0, :, :, columns].reshape(768, 128)
            places = (2 * y + core) * 48 + col_p
            valid = (col_b == row_b) & (places < limit)
            scores.append(jnp.where(valid, dot_t(q, keys), LOWEST))
        top = jnp.maximum(*[jnp.max(s, axis=1, keepdims=True) for s in scores])
        top = top.astype(bf16).astype(f32)
        total = jnp.zeros((128, 1), f32)
        summed = jnp.zeros((128, 128), f32)
        for core in range(2):
            weights = jnp.exp2((scores[core] - top) * FACTOR)
            total += jnp.sum(weights, axis=1, keepdims=True)
            values = dbuf[core, 1, :, :, columns].reshape(768, 128)
            summed += jnp.dot(weights.astype(bf16), values, preferred_element_type=f32)
        stats = jnp.where(lane < 64, top, total).astype(bf16)
        summed = summed.astype(bf16)
        for n in range(2):
            dec_send[2 * g + n, 0] = summed[64 * n : 64 * n + 64]
            dec_send[2 * g + n, 1] = stats[64 * n : 64 * n + 64]
    dec_copies = []
    for j in range(4):
        copy = remote(dec_send.at[j], dec_recv.at[y], dec_ssem.at[j], dec_rsem.at[y], 2 * (4 * c + j) + 1)
        dec_copies.append(copy)
        stays = (c == 1) & (y == 4 + j)

        @pl.when(stays)
        def _():
            dec_recv[y] = dec_send[j]

        @pl.when(jnp.logical_not(stays))
        def _():
            copy.start()

    for steps in (1, -1, -4):
        take_kv(steps)
    col = iota((1, 1536), 1)
    owner = (col * 683) >> 16
    place = col - 96 * owner
    locals_[0].wait()
    start = start_ref[0]
    from_history = jnp.where(owner * span + place < start, -1, NEVER)
    from_prompt = jnp.where(place < span + entries, owner * entries + place - span, NEVER)
    first_row = jnp.where(place < span, from_history, from_prompt)
    row32 = iota((128, 1), 0) & 31

    for n in (2, 4, 5, 6, 7):
        locals_[n].wait()
    for copy in pairs[1:5]:
        copy.wait_recv()
    for k in range(CHIPS):
        wait_kv(2 * ((y + k) % CHIPS) + 1 - c)

    def decode_rows(slot):
        for s in range(CHIPS):
            @pl.when(jnp.logical_not((y == s) & (y >= 4)))
            def _():
                pltpu.make_async_copy(dec_send.at[0], dec_recv.at[s], dec_rsem.at[s]).wait()
        query = qbuf[:, rows : rows + 16, :].astype(f32)
        key = fresh[0].astype(f32)
        value = fresh[1].astype(f32)
        own = jnp.sum(query * key[None], axis=-1, keepdims=True).reshape(64, 1)
        value = jnp.concatenate([value] * 4, axis=0)
        tops = [dec_recv[s, 1, :, 0:1].astype(f32) for s in range(CHIPS)]
        top = own
        for s in range(CHIPS):
            top = jnp.maximum(top, tops[s])
        own_weight = jnp.exp2((own - top) * FACTOR)
        total = own_weight
        summed = own_weight.astype(bf16).astype(f32) * value
        for s in range(CHIPS):
            factor = jnp.exp2((tops[s] - top) * FACTOR)
            total += factor * dec_recv[s, 1, :, 64:65].astype(f32)
            summed += factor * dec_recv[s, 0].astype(f32)
        out = (summed / total).astype(bf16)
        for n in range(4):
            att[slot, 16:32, 128 * n : 128 * n + 128] = out[16 * n : 16 * n + 16]

    def attend(d, slot):
        row = pl.multiple_of(64 * d + 32 * c, 32)
        q = qbuf[:, pl.ds(row, 32), :].reshape(128, 128)
        keys = kv[:, 0].reshape(1536, 128)
        values = kv[:, 1].reshape(1536, 128)
        scores = jnp.where(first_row <= row + row32, dot_t(q, keys), LOWEST)
        top = jnp.max(scores, axis=1, keepdims=True)
        weights = jnp.exp2((scores - top) * FACTOR)
        total = jnp.sum(weights, axis=1, keepdims=True)
        summed = jnp.dot(weights.astype(bf16), values, preferred_element_type=f32)
        out = (summed / total).astype(bf16)
        for n in range(4):
            att[slot, :, 128 * n : 128 * n + 128] = out[32 * n : 32 * n + 32]

        @pl.when((d == CHIPS - 1) & (c == 1))
        def _():
            decode_rows(slot)

    def project(sub):
        return jnp.dot(att[0], wbuf[sub], preferred_element_type=f32)

    right, left = 2 * ((y + 1) % CHIPS) + c, 2 * ((y + 7) % CHIPS) + c

    def rs_copy(way, step, sub):
        return remote(
            rs_send.at[way, step, sub], rs_recv.at[way, step, sub],
            rs_ssem.at[way, step, sub], rs_rsem.at[way, step, sub], right if way == 0 else left,
        )

    locals_[8].wait()
    attend((y + 4) % CHIPS, 0)
    for copy in own_weights:
        copy.wait()
    for copy in weights_in:
        copy.wait_recv()

    def first_body(j, carry):
        for way in range(2):
            sub = j + HALF * way
            rs_send[way, 0, sub] = project(sub).astype(bf16)
            rs_copy(way, 0, sub).start()
        return carry
    lax.fori_loop(0, HALF, first_body, 0)

    def step_body(step, carry):
        away = 4 - step

        def attend_body(j, carry):
            attend((y + CHIPS + away * (1 - 2 * j)) % CHIPS, j)
            return carry
        lax.fori_loop(0, 2, attend_body, 0)

        def own_body(sub, carry):
            both = att[...].reshape(64, 512)
            own[sub] = jnp.dot(both, wbuf[sub], preferred_element_type=f32)
            return carry
        lax.fori_loop(0, SUBS, own_body, 0)

        def sub_body(j, carry):
            for way in range(2):
                sub = (j + HALF) % SUBS if way == 0 else j

                @pl.when((step > 1) | (j >= HALF))
                def _():
                    rs_copy(way, step - 1, sub).wait_recv()

                added = own[sub, 32 * way : 32 * way + 32] + rs_recv[way, step - 1, sub].astype(f32)
                rs_send[way, step, sub] = added.astype(bf16)
                rs_copy(way, step, sub).start()
            return carry
        return lax.fori_loop(0, SUBS, sub_body, carry)

    lax.fori_loop(1, 4, step_body, 0)

    attend(y, 0)
    locals_[10].wait()

    def mine_body(sub, carry):
        hid[:, lanes(sub, width)] = project(sub) + resbuf[:, lanes(sub, width)].astype(f32)
        return carry
    lax.fori_loop(0, SUBS, mine_body, 0)

    def last_body(j, carry):
        for way in range(2):
            sub = (j + HALF) % SUBS if way == 0 else j
            rs_copy(way, 3, sub).wait_recv()
            hid[:, lanes(sub, width)] += rs_recv[way, 3, sub].astype(f32)
        return carry
    lax.fori_loop(0, SUBS, last_body, 0)

    for copy in qd_copies + kv_copies + pairs:
        copy.wait_send()

    @pl.when(c != half)
    def _():
        qd_pair.wait_send()

    for j in range(4):
        @pl.when(jnp.logical_not((c == 1) & (y == 4 + j)))
        def _():
            dec_copies[j].wait_send()

    for j in range(HALF):
        for way in range(2):
            rs_copy(way, 0, j + HALF * way).wait_send()

    def rs_done(n, carry):
        for way in range(2):
            rs_copy(way, 1 + n // SUBS, n % SUBS).wait_send()
        return carry
    lax.fori_loop(0, 3 * SUBS, rs_done, 0)


def finish(hid, gain, out_res, out_norm):
    hidden = hid[...]
    out_res[...] = hidden.astype(bf16)
    mean_square = jnp.sum(hidden * hidden, axis=1, keepdims=True) * (1.0 / hidden.shape[1])
    out_norm[...] = (hidden * lax.rsqrt(mean_square + 1e-05) * gain[...]).astype(bf16)


def per_device(
    prompt_queries, prompt_entries, history_cache, decode_queries, decode_entries, decode_cache,
    decode_lengths, prompt_start, out_weight, residual, norm_gain,
):
    hbm = pl.BlockSpec(memory_space=pltpu.HBM)
    vmem = pl.BlockSpec(memory_space=pltpu.VMEM)
    span = history_cache.shape[1]
    entries = prompt_entries.shape[1]
    tokens, width = residual.shape
    dma = pltpu.SemaphoreType.DMA
    hidden = pl.pallas_call(
        kernel,
        out_shape=jax.ShapeDtypeStruct((tokens, width), f32),
        in_specs=[hbm] * 10,
        out_specs=vmem,
        scratch_shapes=[
            pltpu.SMEM(prompt_start.shape, jnp.int32),
            pltpu.SMEM(decode_lengths.shape, jnp.int32),
            pltpu.VMEM((4, 2, span + 32, 128), bf16),
            pltpu.VMEM((entries, 2, 512), bf16),
            pltpu.VMEM((GROUP, 2, span + 32, 128), bf16),
            pltpu.VMEM((4, 512, 128), bf16),
            pltpu.VMEM((2, 2, 16, 48, 256), bf16),
            pltpu.VMEM((8, 16, 256), bf16),
            pltpu.VMEM((SUBS, 512, width // SUBS), bf16),
            pltpu.VMEM((tokens, width), bf16),
            pltpu.VMEM((2, 16, 128), bf16),
            pltpu.VMEM((4, 2, 64, 128), bf16),
            pltpu.VMEM((CHIPS, 2, 64, 128), bf16),
            pltpu.VMEM((2, 32, 512), bf16),
            pltpu.VMEM((SUBS, 64, width // SUBS), f32),
            pltpu.VMEM((2, 4, SUBS, 32, width // SUBS), bf16),
            pltpu.VMEM((2, 4, SUBS, 32, width // SUBS), bf16),
            dma((15 + SUBS,)), dma((8,)), dma((8,)), dma((16,)), dma((16,)), dma((5 + SUBS,)), dma((5 + SUBS,)),
            dma((4,)), dma((8,)), dma((2, 4, SUBS)), dma((2, 4, SUBS)), pltpu.SemaphoreType.REGULAR,
        ],
        compiler_params=pltpu.CompilerParams(collective_id=0, has_side_effects=True),
    )(
        prompt_start, decode_lengths, prompt_queries, prompt_entries.transpose(1, 0, 2), history_cache,
        decode_queries, decode_entries, decode_cache, out_weight, residual,
    )
    shape = jax.ShapeDtypeStruct(residual.shape, residual.dtype)
    return pl.pallas_call(
        finish, out_shape=(shape, shape), in_specs=[vmem, vmem], out_specs=(vmem, vmem),
    )(hidden, norm_gain.reshape(1, -1))


def solution(mesh):
    placed = (
        P("rep", "tp"),
        P("rep", "tp", None),
        P("rep", "tp", None),
        P("rep", "tp"),
        P("rep", None, None),
        P("rep", None, "tp", None),
        P("rep"),
        P("rep"),
        P("tp", None),
        P("tp", "rep"),
        P(None),
    )
    return jax.shard_map(
        per_device, mesh=mesh, in_specs=placed, out_specs=(P("tp", "rep"), P("tp", "rep")),
        check_vma=False,
    )
```
